32 devices in a mesh: row: 8 (over y, x, core), col: 4 (over z).
Axes of the slice: x: 2, y: 2, z: 4, core: 2. Of those that a mesh axis runs over, the one named last changes fastest.
Arguments:
- species: float32 [2, 256, 256, 128], P(None, None, 'row', 'col'), may hold values from -6 to 6
- coupling: float32 [2, 2], replicated, may hold values from -4 to 4
- symbol_x: float32 [256], replicated, may hold values from 0.3 to 3
- symbol_y: float32 [256], replicated, may hold values from 0.3 to 3
- symbol_z: float32 [128], replicated, may hold values from 0.3 to 3
Outputs:
- modes: float32 [2, 256, 256, 128], P(None, 'row', 'col')
The draws below stay inside these ranges and needn't reach their ends.
All inputs are finite; a program needn't handle non-finite values.
Results may differ from the reference program's by a relative error of at most 0.000078.
Values sent between devices are 32-bit elements.
A program may use at most 128 MiB of HBM per device.

```python
import jax
import jax.numpy as jnp
from jax import lax

GRID_X = 256
GRID_Y = 256
GRID_Z = 128
FIELDS = 2


def block_scale(own_key, shape, cuts, low, top_value):
    level, own = 1.0, jax.random.fold_in(own_key, 6)
    for position, shards_of in cuts:
        draws = jnp.exp(jax.random.uniform(jax.random.fold_in(own, position), (shards_of,), jnp.float32, low / len(cuts), top_value / len(cuts)))
        level = level * jnp.repeat(draws, shape[position] // shards_of).reshape([-1 if axis == position else 1 for axis in range(len(shape))])
    return level


def scatter_about(key, extent, width, limit, shards=(), kind=jnp.bfloat16):
    values = width * jax.random.normal(key, extent, jnp.float32)
    if shards:
        values = values * block_scale(key, extent, shards, -0.22, 0.18)
    return jnp.clip(values, -limit, limit).astype(kind)


def setup_inputs(seed: int = 0) -> dict:
    seeds = jax.random.split(jax.random.key(seed), 6)
    species = scatter_about(seeds[0], (FIELDS, GRID_X, GRID_Y, GRID_Z), 1.0, 6.0, ((2, 8), (3, 4)), jnp.float32)
    coupling = scatter_about(seeds[1], (FIELDS, FIELDS), 0.7, 4.0, (), jnp.float32)
    symbol_x = jnp.clip(jax.random.uniform(seeds[2], (GRID_X,), jnp.float32, 0.3, 3.0), 0.3, 3.0)
    symbol_y = jnp.clip(jax.random.uniform(seeds[3], (GRID_Y,), jnp.float32, 0.3, 3.0), 0.3, 3.0)
    symbol_z = jnp.clip(jax.random.uniform(seeds[4], (GRID_Z,), jnp.float32, 0.3, 3.0), 0.3, 3.0)
    return {"species": species, "coupling": coupling, "symbol_x": symbol_x, "symbol_y": symbol_y, "symbol_z": symbol_z}


def mode_table(count):
    rank = jnp.arange(count)
    angle = (jnp.pi / (count + 1)) * (((rank[:, None] + 1) * (rank[None, :] + 1)) % (2 * count + 2)).astype(jnp.float32)
    return jnp.sin(angle) * (2.0 / (count + 1)) ** 0.5


def transform_dim(values, dim):
    moved = jnp.tensordot(values, mode_table(values.shape[dim]), axes=([dim], [0]), precision=lax.Precision.HIGHEST)
    return jnp.moveaxis(moved, -1, dim)


def reference(species, coupling, symbol_x, symbol_y, symbol_z):
    modes = species
    modes = transform_dim(modes, 1)
    modes = transform_dim(modes, 2)
    modes = transform_dim(modes, 3)
    symbol = symbol_x[:, None, None] + symbol_y[None, :, None] + symbol_z[None, None, :]
    weight_xyz = 1.0 / (1.0 + symbol)
    mixed_fields = jnp.einsum("ab,bxyz->axyz", coupling, modes, precision=lax.Precision.HIGHEST)
    modes = weight_xyz * modes + (1.0 - weight_xyz) * mixed_fields
    return modes
```

```python
import functools

import jax
import jax.numpy as jnp
import numpy as np
from jax import lax
from jax.experimental import pallas as pl
from jax.experimental.pallas import tpu as pltpu
from jax.sharding import PartitionSpec as P

MESH = pl.DeviceIdType.MESH
LANES = 128
SUB = 8
DEPTH = LANES // SUB
HELD = 4


def mode_table(count):
    rank = np.arange(1, count + 1)
    angle = np.pi / (count + 1) * ((rank[:, None] * rank[None, :]) % (2 * count + 2))
    return (np.sin(angle) * np.sqrt(2.0 / (count + 1))).astype(np.float32)


def halves_of(table):
    high = table.astype(jnp.bfloat16)
    low = (table - high.astype(np.float32)).astype(jnp.bfloat16)
    return high, low


def halves(values):
    high = values.astype(jnp.bfloat16)
    low = (values - high.astype(jnp.float32)).astype(jnp.bfloat16)
    return high, low


def partner(me, step, count):
    if count & (count - 1):
        return lax.rem(me + step, count)
    other, bit = me, 1
    while bit < count:
        if step & bit:
            other = other + bit * (1 - 2 * lax.rem(me // bit, 2))
        bit *= 2
    return other


def swap_groups(parts):
    parts = list(parts)
    count = len(parts)
    width = LANES // count
    lane = lax.broadcasted_iota(jnp.int32, parts[0].shape, 1)
    step = count // 2
    while step:
        keep = lax.rem(lane // (width * step), 2) == 0
        for first in range(count):
            if first & step:
                continue
            a, b = parts[first], parts[first + step]
            parts[first] = jnp.where(keep, a, pltpu.roll(b, width * step, 1))
            parts[first + step] = jnp.where(keep, pltpu.roll(a, LANES - width * step, 1), b)
        step //= 2
    return parts


def kernel(sizes, c_hbm, sx_hbm, a_hbm, hx_hbm, hy_hbm, hz_hbm, sy_hbm, sz_hbm, o_ref,
           c_ref, sx_ref, sy_ref, sz_ref, a_ref, hx_ref, hy_ref, hz_ref, sy_rows, m_ref,
           t_ref, r_ref, v_ref, w_ref,
           load_a, load_h, load_s, send_row, recv_row, send_col, recv_col):
    rows, cols, fields, nx, ny, nz = sizes
    share_y = ny // cols
    near_y = ny // rows
    depths = nz // cols // DEPTH
    blocks = near_y // SUB
    chunks = nx // rows // SUB
    stages = fields * depths
    total = stages * chunks
    slab = blocks * SUB
    span = rows * SUB
    row, col = lax.axis_index("row"), lax.axis_index("col")
    per_dot = 2
    width = per_dot * LANES
    pieces = blocks // per_dot

    def load(s, n):
        f, d = s // depths, s % depths
        lines = width // DEPTH
        return pltpu.make_async_copy(
            a_hbm.at[f, pl.ds(n * lines, lines), pl.ds(d * DEPTH, DEPTH)],
            a_ref.at[s, pl.ds(n * lines, lines)], load_a.at[s, n])

    tables = [pltpu.make_async_copy(src, dst, load_h.at[n]) for n, (src, dst) in enumerate(
        ((hx_hbm, hx_ref), (hy_hbm, hy_ref), (hz_hbm, hz_ref)))]
    smalls = [pltpu.make_async_copy(src, dst, load_s.at[n]) for n, (src, dst) in enumerate(
        ((c_hbm, c_ref), (sx_hbm, sx_ref), (sy_hbm, sy_ref), (sz_hbm, sz_ref)))]
    barrier = pltpu.get_barrier_semaphore()
    tables[0].start()
    for n in range(pieces):
        load(0, n).start()
    for step in range(1, rows):
        pl.semaphore_signal(barrier, inc=1, device_id={"row": partner(row, step, rows)}, device_id_type=MESH)
    for step in range(1, cols):
        pl.semaphore_signal(barrier, inc=1, device_id={"col": partner(col, step, cols)}, device_id_type=MESH)
    for s in range(1, stages):
        for n in range(pieces):
            load(s, n).start()
    tables[1].start()
    tables[2].start()
    for small in smalls:
        small.start()

    def row_copy(i, step):
        to = partner(row, step, rows)
        return pltpu.make_async_remote_copy(
            src_ref=t_ref.at[i, to], dst_ref=r_ref.at[i, pl.ds(row * slab, slab)],
            send_sem=send_row.at[0], recv_sem=recv_row.at[i],
            device_id={"row": to}, device_id_type=MESH)

    def col_copy(i, step):
        to = partner(col, step, cols)
        return pltpu.make_async_remote_copy(
            src_ref=v_ref.at[i, to], dst_ref=w_ref.at[i, col],
            send_sem=send_col.at[0], recv_sem=recv_col.at[i],
            device_id={"col": to}, device_id_type=MESH)

    def landed(ref, sem):
        pltpu.make_async_copy(ref, ref, sem).wait()

    def x_step(s, low_j, top_j, waits):
        for n in range(pieces):
            if waits:
                load(s, n).wait()
            lines = width // DEPTH
            high, low = halves(a_ref[s, n * lines:(n + 1) * lines].reshape(width, nx))
            part = lax.dot_general(
                hx_ref[low_j * span:top_j * span, :], jnp.concatenate([high, high, low], axis=1),
                (((1,), (1,)), ((), ())), preferred_element_type=jnp.float32)
            part = part.reshape(top_j - low_j, rows, SUB, width)
            for j in range(low_j, top_j):
                for b in range(per_dot):
                    at = (n * per_dot + b) * SUB
                    t_ref[s * chunks + j, :, at:at + SUB, :] = part[
                        j - low_j, :, :, b * LANES:(b + 1) * LANES]

    def x_send(s, low_j, top_j):
        for j in range(low_j, top_j):
            i = s * chunks + j
            for step in range(rows - 1, 0, -1):
                row_copy(i, step).start()
            r_ref[i, pl.ds(pl.multiple_of(row * slab, slab), slab), :] = t_ref[i, row]

    tables[0].wait()
    x_step(0, 0, 1, True)
    pl.semaphore_wait(barrier, rows + cols - 2)
    x_send(0, 0, 1)
    x_step(0, 1, chunks, False)
    x_send(0, 1, chunks)

    def x_stage(s, carry):
        x_step(s, 0, chunks, True)
        x_send(s, 0, chunks)
        return carry

    lax.fori_loop(1, stages, x_stage, 0)

    tables[1].wait()

    def held(step):
        to = partner(col, step, cols)
        late = jnp.logical_and(col * 2 >= cols, jnp.logical_and(to * 2 < cols, to * 4 >= cols))
        return jnp.where(late, HELD, 0)

    def col_send(i):
        for step in range(cols - 1, 0, -1):
            k = i - held(step)

            @pl.when(jnp.logical_and(k >= 0, k < total))
            def _():
                col_copy(k, step).start()

    def y_step(i, carry):
        landed(r_ref.at[i, pl.ds(0, (rows - 1) * slab)], recv_row.at[i])
        parts = [r_ref[i, pl.ds(g, rows * blocks, stride=SUB), :] for g in range(SUB)]
        high, low = halves(jnp.concatenate(swap_groups(parts), axis=0))
        got = jnp.dot(hy_ref[...], jnp.concatenate([high, high, low], axis=0),
                      preferred_element_type=jnp.float32)
        v_ref[i] = got.reshape(cols, share_y, LANES)
        col_send(i)
        w_ref[i, col] = v_ref[i, col]
        return carry

    lax.fori_loop(0, total, y_step, 0)

    def late_send(i, carry):
        col_send(i)
        return carry

    lax.fori_loop(total, total + HELD, late_send, 0)

    tables[2].wait()
    for small in smalls:
        small.wait()
    for n in range(ny // LANES):
        at = slice(n * LANES, (n + 1) * LANES)
        sy_rows[at, :] = jnp.broadcast_to(sy_ref[:, at], (LANES, LANES)).T

    def modes_of(f, j):
        parts = []
        for d in range(depths):
            i = (f * depths + d) * chunks + j
            landed(w_ref.at[i, pl.ds(0, cols - 1)], recv_col.at[i])
        tiles = []
        parts = [w_ref[(f * depths + p % depths) * chunks + j, p // depths] for p in range(cols * depths)]
        for p in range(0, cols * depths, SUB):
            tiles.append(swap_groups(parts[p:p + SUB]))
        lines = [jnp.concatenate([tile[k] for tile in tiles], axis=1) for k in range(SUB)]
        high, low = halves(jnp.concatenate(lines, axis=0))
        got = jnp.dot(jnp.concatenate([high, low], axis=1), hz_ref[...],
                      preferred_element_type=jnp.float32)
        return got[:, :nz] + got[:, nz:]

    def z_step(i, carry):
        m_ref[i] = modes_of(i // chunks, lax.rem(i, chunks))
        return carry

    lax.fori_loop(0, (fields - 1) * chunks, z_step, 0)

    def last_step(j, carry):
        last = modes_of(fields - 1, j)
        lines_y = sy_rows[pl.ds(col * share_y, share_y), :]
        lines_y = jnp.concatenate([lines_y] * (nz // LANES), axis=1) + sz_ref[...]
        for k in range(SUB):
            at = slice(k * share_y, (k + 1) * share_y)
            weight = 1.0 / (1.0 + (sx_ref[row * (chunks * SUB) + j * SUB + k] + lines_y))
            old = [m_ref[f * chunks + j, at, :] for f in range(fields - 1)] + [last[at, :]]
            for f in range(fields):
                mixed = c_ref[f, 0] * old[0]
                for b in range(1, fields):
                    mixed = mixed + c_ref[f, b] * old[b]
                o_ref[f, j * SUB + k] = weight * old[f] + (1.0 - weight) * mixed
        return carry

    lax.fori_loop(0, chunks, last_step, 0)

    landed(t_ref.at[pl.ds(0, total), pl.ds(0, rows - 1)], send_row.at[0])
    landed(v_ref.at[pl.ds(0, total), pl.ds(0, cols - 1)], send_col.at[0])


def local(rows, cols, species, coupling, symbol_x, symbol_y, symbol_z):
    fields, nx, near_y, near_z = species.shape
    ny, nz = near_y * rows, near_z * cols
    share_x, share_y = nx // rows, ny // cols
    depths, blocks, chunks = near_z // DEPTH, near_y // SUB, share_x // SUB
    stages = fields * depths
    total = stages * chunks

    order = np.arange(nx).reshape(rows, chunks, SUB).transpose(1, 0, 2).reshape(-1)
    high, low = halves_of(mode_table(nx)[order])
    hx = np.concatenate([high, low, high], axis=1)
    order = np.arange(ny).reshape(rows, blocks, SUB).transpose(2, 0, 1).reshape(-1)
    high, low = halves_of(mode_table(ny)[:, order])
    hy = np.concatenate([high, low, high], axis=1)
    high, low = halves_of(mode_table(nz))
    hz = np.concatenate([np.concatenate([high, low], axis=1),
                         np.concatenate([high, np.zeros_like(low)], axis=1)], axis=0)

    lines = jnp.transpose(species, (0, 2, 3, 1))
    vmem = pl.BlockSpec(memory_space=pltpu.VMEM)
    hbm = pl.BlockSpec(memory_space=pltpu.HBM)
    dma = pltpu.SemaphoreType.DMA
    f32 = jnp.float32
    return pl.pallas_call(
        functools.partial(kernel, (rows, cols, fields, nx, ny, nz)),
        out_shape=pltpu.VMEM((fields, share_x, share_y, nz), f32),
        in_specs=[hbm] * 8,
        out_specs=vmem,
        scratch_shapes=[
            pltpu.SMEM(coupling.shape, f32),
            pltpu.SMEM(symbol_x.shape, f32),
            pltpu.VMEM((1, ny), f32),
            pltpu.VMEM((1, nz), f32),
            pltpu.VMEM((stages, near_y, DEPTH, nx), f32),
            pltpu.VMEM(hx.shape, hx.dtype),
            pltpu.VMEM(hy.shape, hy.dtype),
            pltpu.VMEM(hz.shape, hz.dtype),
            pltpu.VMEM((ny, LANES), f32),
            pltpu.VMEM((max((fields - 1) * chunks, 1), SUB * share_y, nz), f32),
            pltpu.VMEM((total, rows, blocks * SUB, LANES), f32),
            pltpu.VMEM((total, rows * blocks * SUB, LANES), f32),
            pltpu.VMEM((total, cols, share_y, LANES), f32),
            pltpu.VMEM((total, cols, share_y, LANES), f32),
            dma((stages, blocks // 2)), dma((3,)), dma((4,)),
            dma((1,)), dma((total,)), dma((1,)), dma((total,)),
        ],
        compiler_params=pltpu.CompilerParams(
            collective_id=0, has_side_effects=True, vmem_limit_bytes=56 * 2**20),
    )(coupling, symbol_x, lines, jnp.asarray(hx), jnp.asarray(hy), jnp.asarray(hz),
      symbol_y[None, :], symbol_z[None, :])


def solution(mesh):
    return jax.shard_map(
        functools.partial(local, mesh.shape["row"], mesh.shape["col"]),
        mesh=mesh,
        in_specs=(P(None, None, "row", "col"), P(), P(), P(), P()),
        out_specs=P(None, "row", "col", None),
        check_vma=False,
    )
```

```python
import functools

import jax
import jax.numpy as jnp
import numpy as np
from jax import lax
from jax.experimental import pallas as pl
from jax.experimental.pallas import tpu as pltpu
from jax.sharding import PartitionSpec as P

MESH = pl.DeviceIdType.MESH
LANES = 128
SUB = 8
DEPTH = LANES // SUB
FIRST = 3
HELD = 5
RELAY = 4


def mode_table(count):
    rank = np.arange(1, count + 1)
    angle = np.pi / (count + 1) * ((rank[:, None] * rank[None, :]) % (2 * count + 2))
    return (np.sin(angle) * np.sqrt(2.0 / (count + 1))).astype(np.float32)


def halves_of(table):
    high = table.astype(jnp.bfloat16)
    low = (table - high.astype(np.float32)).astype(jnp.bfloat16)
    return high, low


def halves(values):
    high = values.astype(jnp.bfloat16)
    low = (values - high.astype(jnp.float32)).astype(jnp.bfloat16)
    return high, low


def partner(me, step, count):
    if count & (count - 1):
        return lax.rem(me + step, count)
    other, bit = me, 1
    while bit < count:
        if step & bit:
            other = other + bit * (1 - 2 * lax.rem(me // bit, 2))
        bit *= 2
    return other


def swap_groups(parts):
    parts = list(parts)
    count = len(parts)
    width = LANES // count
    lane = lax.broadcasted_iota(jnp.int32, parts[0].shape, 1)
    step = count // 2
    while step:
        keep = lax.rem(lane // (width * step), 2) == 0
        for first in range(count):
            if first & step:
                continue
            a, b = parts[first], parts[first + step]
            parts[first] = jnp.where(keep, a, pltpu.roll(b, width * step, 1))
            parts[first + step] = jnp.where(keep, pltpu.roll(a, LANES - width * step, 1), b)
        step //= 2
    return parts


def modes_of(f, j, chunks, depths, w_ref, hz_ref):
    cols, nz = w_ref.shape[1], hz_ref.shape[1] // 2
    parts = [w_ref[(f * depths + p % depths) * chunks + j, p // depths] for p in range(cols * depths)]
    tiles = [swap_groups(parts[p:p + SUB]) for p in range(0, cols * depths, SUB)]
    lines = [jnp.concatenate([tile[k] for tile in tiles], axis=1) for k in range(SUB)]
    high, low = halves(jnp.concatenate(lines, axis=0))
    got = jnp.dot(jnp.concatenate([high, low], axis=1), hz_ref[...],
                  preferred_element_type=jnp.float32)
    return got[:, :nz] + got[:, nz:]


def kernel(sizes, c_hbm, sx_hbm, a_hbm, hx_hbm, hy_hbm, hz_hbm, sy_hbm, sz_hbm,
           o_ref, g_ref, w_ref, hz_ref,
           c_ref, sx_ref, sy_ref, sz_ref, a_ref, hx_ref, hy_ref, sy_rows, m_ref,
           t_ref, r_ref, v_ref, q_ref, u_ref, x_ref,
           load_a, load_h, load_s, send_row, recv_row, send_col, recv_col, send_x, recv_x):
    rows, cols, fields, nx, ny, nz = sizes
    share_y = ny // cols
    near_y = ny // rows
    depths = nz // cols // DEPTH
    blocks = near_y // SUB
    chunks = nx // rows // SUB
    stages = fields * depths
    total = stages * chunks
    slab = blocks * SUB
    span = rows * SUB
    row, col = lax.axis_index("row"), lax.axis_index("col")
    chips, half = rows // 2, cols // 2
    chip, side = row // 2, lax.rem(row, 2)
    mirror = cols - 1 - col
    per_dot = 2
    width = per_dot * LANES
    pieces = blocks // per_dot

    def load(s, n):
        f, d = s // depths, s % depths
        lines = width // DEPTH
        return pltpu.make_async_copy(
            a_hbm.at[f, pl.ds(n * lines, lines), pl.ds(d * DEPTH, DEPTH)],
            a_ref.at[s, pl.ds(n * lines, lines)], load_a.at[s, n])

    tables = [pltpu.make_async_copy(src, dst, load_h.at[n]) for n, (src, dst) in enumerate(
        ((hx_hbm.at[pl.ds(0, span)], hx_ref.at[pl.ds(0, span)]),
         (hx_hbm.at[pl.ds(span, nx - span)], hx_ref.at[pl.ds(span, nx - span)]),
         (hy_hbm, hy_ref), (hz_hbm, hz_ref)))]
    smalls = [pltpu.make_async_copy(src, dst, load_s.at[n]) for n, (src, dst) in enumerate(
        ((c_hbm, c_ref), (sx_hbm, sx_ref), (sy_hbm, sy_ref), (sz_hbm, sz_ref)))]
    barrier = pltpu.get_barrier_semaphore()
    tables[0].start()
    for n in range(pieces):
        load(0, n).start()
    for step in range(1, rows):
        pl.semaphore_signal(barrier, inc=1, device_id={"row": partner(row, step, rows)}, device_id_type=MESH)
    for step in range(1, cols):
        pl.semaphore_signal(barrier, inc=1, device_id={"col": partner(col, step, cols)}, device_id_type=MESH)
    tables[1].start()
    for s in range(1, stages):
        for n in range(pieces):
            load(s, n).start()
    tables[2].start()
    tables[3].start()
    for small in smalls:
        small.start()

    def row_copy(i, to_chip, to_side):
        return pltpu.make_async_remote_copy(
            src_ref=t_ref.at[i, to_side, to_chip], dst_ref=r_ref.at[i, pl.ds(row * slab, slab)],
            send_sem=send_row.at[0], recv_sem=recv_row.at[i],
            device_id={"row": 2 * to_chip + to_side}, device_id_type=MESH)

    def cross_copy():
        return pltpu.make_async_remote_copy(
            src_ref=t_ref.at[0, 0], dst_ref=q_ref, send_sem=send_x.at[0], recv_sem=recv_x.at[0],
            device_id={"col": mirror}, device_id_type=MESH)

    def relay_copy(to_chip):
        return pltpu.make_async_remote_copy(
            src_ref=q_ref.at[to_chip], dst_ref=u_ref.at[pl.ds(row * slab, slab)],
            send_sem=send_x.at[1], recv_sem=recv_x.at[1],
            device_id={"row": 2 * to_chip}, device_id_type=MESH)

    def relay_col_copy(to):
        return pltpu.make_async_remote_copy(
            src_ref=x_ref.at[to], dst_ref=w_ref.at[0, mirror],
            send_sem=send_x.at[2], recv_sem=recv_x.at[2],
            device_id={"col": to}, device_id_type=MESH)

    def col_copy(i, step):
        to = partner(col, step, cols)
        return pltpu.make_async_remote_copy(
            src_ref=v_ref.at[i, to], dst_ref=w_ref.at[i, col],
            send_sem=send_col.at[0], recv_sem=recv_col.at[i],
            device_id={"col": to}, device_id_type=MESH)

    def landed(ref, sem):
        pltpu.make_async_copy(ref, ref, sem).wait()

    def x_step(s, low_j, top_j, waits):
        for n in range(pieces):
            if waits:
                load(s, n).wait()
            lines = width // DEPTH
            high, low = halves(a_ref[s, n * lines:(n + 1) * lines].reshape(width, nx))
            part = lax.dot_general(
                hx_ref[low_j * span:top_j * span, :], jnp.concatenate([high, high, low], axis=1),
                (((1,), (1,)), ((), ())), preferred_element_type=jnp.float32)
            part = part.reshape(top_j - low_j, 2, chips, SUB, width)
            for j in range(low_j, top_j):
                for b in range(per_dot):
                    at = (n * per_dot + b) * SUB
                    t_ref[s * chunks + j, :, :, at:at + SUB, :] = part[
                        j - low_j, :, :, :, b * LANES:(b + 1) * LANES]

    def x_send(s, low_j, top_j):
        for j in range(low_j, top_j):
            i = s * chunks + j
            for to_side in (1, 0):
                for step in range(chips - 1, 0, -1):
                    row_copy(i, partner(chip, step, chips), to_side).start()
                if low_j == 0 and top_j == 1 and to_side:
                    cross_copy().start()
            row_copy(i, chip, 1 - side).start()
            r_ref[i, pl.ds(pl.multiple_of(row * slab, slab), slab), :] = t_ref[i, side, chip]

    tables[0].wait()
    x_step(0, 0, 1, True)
    pl.semaphore_wait(barrier, rows + cols - 2)
    x_send(0, 0, 1)
    tables[1].wait()
    x_step(0, 1, chunks, False)
    x_send(0, 1, chunks)

    def x_stage(s, carry):
        x_step(s, 0, chunks, True)
        x_send(s, 0, chunks)
        return carry

    lax.fori_loop(1, stages, x_stage, 0)

    tables[2].wait()

    def crosses(step):
        return (partner(col, step, cols) // half) != (col // half)

    def held(step):
        to = partner(col, step, cols)
        late = jnp.logical_and(col * 2 >= cols, jnp.logical_and(to * 2 < cols, to * 4 >= cols))
        return jnp.where(late, HELD, 0)

    def col_send(i):
        for step in range(cols - 1, 0, -1):
            k = i - jnp.where(i < FIRST, 0, held(step))
            crossed = jnp.logical_and(jnp.logical_and(k == 0, side == 0), crosses(step))

            due = jnp.logical_and(jnp.logical_or(i < FIRST, k >= FIRST), k < total)

            @pl.when(jnp.logical_and(due, jnp.logical_not(crossed)))
            def _():
                col_copy(k, step).start()

    def y_modes(ref):
        parts = [ref[pl.ds(g, rows * blocks, stride=SUB), :] for g in range(SUB)]
        high, low = halves(jnp.concatenate(swap_groups(parts), axis=0))
        got = jnp.dot(hy_ref[...], jnp.concatenate([high, high, low], axis=0),
                      preferred_element_type=jnp.float32)
        return got.reshape(cols, share_y, LANES)

    def y_step(i, carry):
        landed(r_ref.at[i, pl.ds(0, (rows - 1) * slab)], recv_row.at[i])
        v_ref[i] = y_modes(r_ref.at[i])
        col_send(i)
        w_ref[i, col] = v_ref[i, col]
        return carry

    def late_send(i, carry):
        col_send(i)
        return carry

    lax.fori_loop(0, RELAY, y_step, 0)

    cross_copy().wait_recv()
    for step in range(chips - 1, 0, -1):
        relay_copy(partner(chip, step, chips)).start()

    @pl.when(side == 1)
    def _():
        relay_copy(chip).start()

    @pl.when(side == 0)
    def _():
        u_ref[pl.ds(pl.multiple_of(row * slab, slab), slab), :] = q_ref[chip]

    lax.fori_loop(RELAY, total, y_step, 0)

    lax.fori_loop(total, total + HELD, late_send, 0)

    @pl.when(side == 0)
    def _():
        landed(u_ref.at[pl.ds(0, (rows - 1) * slab)], recv_x.at[1])
        x_ref[...] = y_modes(u_ref)
        base = (col // half) * half
        for step in range(1, half):
            relay_col_copy(base + lax.rem(col - base + step, half)).start()
        w_ref[0, mirror] = x_ref[col]

    tables[3].wait()
    for small in smalls:
        small.wait()
    for n in range(ny // LANES):
        at = slice(n * LANES, (n + 1) * LANES)
        sy_rows[at, :] = jnp.broadcast_to(sy_ref[:, at], (LANES, LANES)).T

    def arrive(f, j):
        for d in range(depths):
            i = (f * depths + d) * chunks + j
            whole = jnp.logical_or(i > 0, side == 1)

            @pl.when(whole)
            def _():
                landed(w_ref.at[i, pl.ds(0, cols - 1)], recv_col.at[i])

            if half > 1:
                @pl.when(jnp.logical_not(whole))
                def _():
                    landed(w_ref.at[i, pl.ds(0, half - 1)], recv_col.at[i])
                    landed(w_ref.at[i, pl.ds(0, half - 1)], recv_x.at[2])

    def z_step(i, carry):
        f, j = i // chunks, lax.rem(i, chunks)
        arrive(f, j)
        m_ref[i] = modes_of(f, j, chunks, depths, w_ref, hz_ref)
        return carry

    lax.fori_loop(0, (fields - 1) * chunks, z_step, 0)

    def blend_step(x, carry):
        j, k = x // SUB, lax.rem(x, SUB)
        lines_y = sy_rows[pl.ds(pl.multiple_of(col * share_y, share_y), share_y), :]
        lines_y = jnp.concatenate([lines_y] * (nz // LANES), axis=1) + sz_ref[...]
        weight = 1.0 / (1.0 + (sx_ref[row * (chunks * SUB) + x] + lines_y))
        at = pl.ds(pl.multiple_of(k * share_y, share_y), share_y)
        old = [m_ref[f * chunks + j, at, :] for f in range(fields - 1)]
        for f in range(fields):
            gain = (1.0 - weight) * c_ref[f, fields - 1]
            g_ref[f, x] = gain if f < fields - 1 else weight + gain
            mixed = jnp.zeros_like(weight)
            for b in range(fields - 1):
                mixed = mixed + c_ref[f, b] * old[b]
            mixed = (1.0 - weight) * mixed
            o_ref[f, x] = weight * old[f] + mixed if f < fields - 1 else mixed
        return carry

    lax.fori_loop(0, chunks * SUB, blend_step, 0)

    def last_step(j, carry):
        arrive(fields - 1, j)
        last = modes_of(fields - 1, j, chunks, depths, w_ref, hz_ref)
        for k in range(SUB):
            for f in range(fields):
                x = j * SUB + k
                o_ref[f, x] = o_ref[f, x] + g_ref[f, x] * last[k * share_y:(k + 1) * share_y, :]
        return carry

    lax.fori_loop(0, chunks - 1, last_step, 0)
    arrive(fields - 1, chunks - 1)

    landed(t_ref.at[pl.ds(0, total), pl.ds(0, 1)], send_row.at[0])
    landed(t_ref.at[pl.ds(0, total), 1, pl.ds(0, chips - 1)], send_row.at[0])
    landed(v_ref.at[pl.ds(0, total - 1), pl.ds(0, cols - 1)], send_col.at[0])
    cross_copy().wait_send()
    landed(q_ref.at[pl.ds(0, chips - 1)], send_x.at[1])

    @pl.when(side == 1)
    def _():
        landed(v_ref.at[0, pl.ds(0, cols - 1)], send_col.at[0])
        landed(q_ref.at[0], send_x.at[1])

    if half > 1:
        @pl.when(side == 0)
        def _():
            landed(v_ref.at[0, pl.ds(0, half - 1)], send_col.at[0])
            landed(x_ref.at[pl.ds(0, half - 1)], send_x.at[2])


def finish(depths, o_ref, g_ref, w_ref, hz_ref, out_hbm, e_ref, sem):
    fields, share_x, share_y, nz = o_ref.shape
    ready = share_x - SUB
    early = [pltpu.make_async_copy(o_ref.at[f, pl.ds(0, ready)], out_hbm.at[f, pl.ds(0, ready)], sem.at[f])
             for f in range(fields)]
    for copy in early:
        copy.start()
    last = modes_of(fields - 1, share_x // SUB - 1, share_x // SUB, depths, w_ref, hz_ref)
    late = []
    for f in range(fields):
        for k in range(SUB):
            x = ready + k
            e_ref[f, k] = o_ref[f, x] + g_ref[f, x] * last[k * share_y:(k + 1) * share_y, :]
        late.append(pltpu.make_async_copy(e_ref.at[f], out_hbm.at[f, pl.ds(ready, SUB)], sem.at[fields + f]))
        late[-1].start()
    for copy in early + late:
        copy.wait()


def local(rows, cols, species, coupling, symbol_x, symbol_y, symbol_z):
    fields, nx, near_y, near_z = species.shape
    ny, nz = near_y * rows, near_z * cols
    share_x, share_y = nx // rows, ny // cols
    depths, blocks, chunks = near_z // DEPTH, near_y // SUB, share_x // SUB
    stages = fields * depths
    total = stages * chunks

    order = np.arange(nx).reshape(rows // 2, 2, chunks, SUB).transpose(2, 1, 0, 3).reshape(-1)
    high, low = halves_of(mode_table(nx)[order])
    hx = np.concatenate([high, low, high], axis=1)
    order = np.arange(ny).reshape(rows, blocks, SUB).transpose(2, 0, 1).reshape(-1)
    high, low = halves_of(mode_table(ny)[:, order])
    hy = np.concatenate([high, low, high], axis=1)
    high, low = halves_of(mode_table(nz))
    hz = np.concatenate([np.concatenate([high, low], axis=1),
                         np.concatenate([high, np.zeros_like(low)], axis=1)], axis=0)

    lines = jnp.transpose(species, (0, 2, 3, 1))
    vmem = pl.BlockSpec(memory_space=pltpu.VMEM)
    hbm = pl.BlockSpec(memory_space=pltpu.HBM)
    dma = pltpu.SemaphoreType.DMA
    f32 = jnp.float32
    out = (fields, share_x, share_y, nz)
    kept = 4 * (2 * fields * share_x * share_y * nz + total * cols * share_y * LANES) + 2 * hz.size
    held = pl.pallas_call(
        functools.partial(kernel, (rows, cols, fields, nx, ny, nz)),
        out_shape=[
            pltpu.VMEM(out, f32),
            pltpu.VMEM(out, f32),
            pltpu.VMEM((total, cols, share_y, LANES), f32),
            pltpu.VMEM(hz.shape, hz.dtype),
        ],
        in_specs=[hbm] * 8,
        out_specs=[vmem] * 4,
        scratch_shapes=[
            pltpu.SMEM(coupling.shape, f32),
            pltpu.SMEM(symbol_x.shape, f32),
            pltpu.VMEM((1, ny), f32),
            pltpu.VMEM((1, nz), f32),
            pltpu.VMEM((stages, near_y, DEPTH, nx), f32),
            pltpu.VMEM(hx.shape, hx.dtype),
            pltpu.VMEM(hy.shape, hy.dtype),
            pltpu.VMEM((ny, LANES), f32),
            pltpu.VMEM((max((fields - 1) * chunks, 1), SUB * share_y, nz), f32),
            pltpu.VMEM((total, 2, rows // 2, blocks * SUB, LANES), f32),
            pltpu.VMEM((total, rows * blocks * SUB, LANES), f32),
            pltpu.VMEM((total, cols, share_y, LANES), f32),
            pltpu.VMEM((rows // 2, blocks * SUB, LANES), f32),
            pltpu.VMEM((rows * blocks * SUB, LANES), f32),
            pltpu.VMEM((cols, share_y, LANES), f32),
            dma((stages, blocks // 2)), dma((4,)), dma((4,)),
            dma((1,)), dma((total,)), dma((1,)), dma((total,)), dma((3,)), dma((3,)),
        ],
        compiler_params=pltpu.CompilerParams(
            collective_id=0, has_side_effects=True, vmem_limit_bytes=60 * 2**20 - kept),
    )(coupling, symbol_x, lines, jnp.asarray(hx), jnp.asarray(hy), jnp.asarray(hz),
      symbol_y[None, :], symbol_z[None, :])
    return pl.pallas_call(
        functools.partial(finish, depths),
        out_shape=jax.ShapeDtypeStruct(out, f32),
        in_specs=[vmem] * 4,
        out_specs=hbm,
        scratch_shapes=[pltpu.VMEM((fields, SUB, share_y, nz), f32), dma((2 * fields,))],
        compiler_params=pltpu.CompilerParams(vmem_limit_bytes=16 * 2**20),
    )(*held)


def solution(mesh):
    return jax.shard_map(
        functools.partial(local, mesh.shape["row"], mesh.shape["col"]),
        mesh=mesh,
        in_specs=(P(None, None, "row", "col"), P(), P(), P(), P()),
        out_specs=P(None, "row", "col", None),
        check_vma=False,
    )
```

```python
import functools

import jax
import jax.numpy as jnp
import numpy as np
from jax import lax
from jax.experimental import pallas as pl
from jax.experimental.pallas import tpu as pltpu
from jax.sharding import PartitionSpec as P

MESH = pl.DeviceIdType.MESH
LANES = 128
SUB = 8
DEPTH = LANES // SUB
HELD = 6
RELAY = 4
AHEAD = 2


def mode_table(count):
    rank = np.arange(1, count + 1)
    angle = np.pi / (count + 1) * ((rank[:, None] * rank[None, :]) % (2 * count + 2))
    return (np.sin(angle) * np.sqrt(2.0 / (count + 1))).astype(np.float32)


def halves_of(table):
    high = table.astype(jnp.bfloat16)
    low = (table - high.astype(np.float32)).astype(jnp.bfloat16)
    return high, low


def halves(values):
    high = values.astype(jnp.bfloat16)
    low = (values - high.astype(jnp.float32)).astype(jnp.bfloat16)
    return high, low


def partner(me, step, count):
    if count & (count - 1):
        return lax.rem(me + step, count)
    other, bit = me, 1
    while bit < count:
        if step & bit:
            other = other + bit * (1 - 2 * lax.rem(me // bit, 2))
        bit *= 2
    return other


def swap_groups(parts):
    parts = list(parts)
    count = len(parts)
    width = LANES // count
    lane = lax.broadcasted_iota(jnp.int32, parts[0].shape, 1)
    step = count // 2
    while step:
        keep = lax.rem(lane // (width * step), 2) == 0
        for first in range(count):
            if first & step:
                continue
            a, b = parts[first], parts[first + step]
            parts[first] = jnp.where(keep, a, pltpu.roll(b, width * step, 1))
            parts[first + step] = jnp.where(keep, pltpu.roll(a, LANES - width * step, 1), b)
        step //= 2
    return parts


def modes_of(f, j, chunks, depths, w_ref, hz_ref):
    cols, nz = w_ref.shape[1], hz_ref.shape[1] // 2
    parts = [w_ref[(f * depths + p % depths) * chunks + j, p // depths] for p in range(cols * depths)]
    tiles = [swap_groups(parts[p:p + SUB]) for p in range(0, cols * depths, SUB)]
    lines = [jnp.concatenate([tile[k] for tile in tiles], axis=1) for k in range(SUB)]
    high, low = halves(jnp.concatenate(lines, axis=0))
    got = jnp.dot(jnp.concatenate([high, low], axis=1), hz_ref[...],
                  preferred_element_type=jnp.float32)
    return got[:, :nz] + got[:, nz:]


def kernel(sizes, c_hbm, sx_hbm, a_hbm, hx_hbm, hy_hbm, hz_hbm, sy_hbm, sz_hbm,
           o_ref, g_ref, w_ref, hz_ref,
           c_ref, sx_ref, sy_ref, sz_ref, a_ref, hx_ref, hy_ref, sy_rows, m_ref,
           t_ref, r_ref, v_ref, q_ref, u_ref, x_ref,
           load_a, load_h, load_s, send_row, recv_row, send_col, recv_col, send_x, recv_x):
    rows, cols, fields, nx, ny, nz = sizes
    share_y = ny // cols
    near_y = ny // rows
    depths = nz // cols // DEPTH
    blocks = near_y // SUB
    chunks = nx // rows // SUB
    stages = fields * depths
    total = stages * chunks
    slab = blocks * SUB
    span = rows * SUB
    row, col = lax.axis_index("row"), lax.axis_index("col")
    chips, half = rows // 2, cols // 2
    chip, side = row // 2, lax.rem(row, 2)
    mirror = cols - 1 - col
    inner = jnp.logical_and(col * 4 >= cols, col * 4 < 3 * cols)
    early = jnp.logical_or(side == 0, inner)
    inners = half // 2
    per_dot = 2
    width = per_dot * LANES
    pieces = blocks // per_dot

    def load(s, n):
        f, d = s // depths, s % depths
        lines = width // DEPTH
        return pltpu.make_async_copy(
            a_hbm.at[f, pl.ds(n * lines, lines), pl.ds(d * DEPTH, DEPTH)],
            a_ref.at[s, pl.ds(n * lines, lines)], load_a.at[s, n])

    tables = [pltpu.make_async_copy(src, dst, load_h.at[n]) for n, (src, dst) in enumerate(
        ((hx_hbm.at[pl.ds(0, span)], hx_ref.at[pl.ds(0, span)]),
         (hx_hbm.at[pl.ds(span, nx - span)], hx_ref.at[pl.ds(span, nx - span)]),
         (hy_hbm, hy_ref), (hz_hbm, hz_ref)))]
    smalls = [pltpu.make_async_copy(src, dst, load_s.at[n]) for n, (src, dst) in enumerate(
        ((c_hbm, c_ref), (sx_hbm, sx_ref), (sy_hbm, sy_ref), (sz_hbm, sz_ref)))]
    barrier = pltpu.get_barrier_semaphore()
    tables[0].start()
    for n in range(pieces):
        load(0, n).start()
    for step in range(1, rows):
        pl.semaphore_signal(barrier, inc=1, device_id={"row": partner(row, step, rows)}, device_id_type=MESH)
    for step in range(1, cols):
        pl.semaphore_signal(barrier, inc=1, device_id={"col": partner(col, step, cols)}, device_id_type=MESH)

    def row_copy(i, to_chip, to_side):
        return pltpu.make_async_remote_copy(
            src_ref=t_ref.at[i, to_side, to_chip], dst_ref=r_ref.at[i, pl.ds(row * slab, slab)],
            send_sem=send_row.at[0], recv_sem=recv_row.at[i],
            device_id={"row": 2 * to_chip + to_side}, device_id_type=MESH)

    def cross_copy(to_side):
        return pltpu.make_async_remote_copy(
            src_ref=t_ref.at[0, to_side], dst_ref=q_ref.at[to_side],
            send_sem=send_x.at[0], recv_sem=recv_x.at[2 + to_side],
            device_id={"col": mirror}, device_id_type=MESH)

    def relay_copy(to_chip, to_side):
        return pltpu.make_async_remote_copy(
            src_ref=q_ref.at[to_side, to_chip], dst_ref=u_ref.at[pl.ds(row * slab, slab)],
            send_sem=send_x.at[1], recv_sem=recv_x.at[0],
            device_id={"row": 2 * to_chip + to_side}, device_id_type=MESH)

    def relay_col_copy(to):
        return pltpu.make_async_remote_copy(
            src_ref=x_ref.at[to], dst_ref=w_ref.at[0, mirror],
            send_sem=send_x.at[2], recv_sem=recv_x.at[1],
            device_id={"col": to}, device_id_type=MESH)

    def col_copy(i, step):
        to = partner(col, step, cols)
        return pltpu.make_async_remote_copy(
            src_ref=v_ref.at[i, to], dst_ref=w_ref.at[i, col],
            send_sem=send_col.at[0], recv_sem=recv_col.at[i],
            device_id={"col": to}, device_id_type=MESH)

    def landed(ref, sem):
        pltpu.make_async_copy(ref, ref, sem).wait()

    def x_step(s, low_j, top_j, waits):
        for n in range(pieces):
            if waits:
                load(s, n).wait()
            lines = width // DEPTH
            high, low = halves(a_ref[s, n * lines:(n + 1) * lines].reshape(width, nx))
            part = lax.dot_general(
                hx_ref[low_j * span:top_j * span, :], jnp.concatenate([high, high, low], axis=1),
                (((1,), (1,)), ((), ())), preferred_element_type=jnp.float32)
            part = part.reshape(top_j - low_j, 2, chips, SUB, width)
            for j in range(low_j, top_j):
                for b in range(per_dot):
                    at = (n * per_dot + b) * SUB
                    t_ref[s * chunks + j, :, :, at:at + SUB, :] = part[
                        j - low_j, :, :, :, b * LANES:(b + 1) * LANES]

    def row_send(i, to_side):
        for step in range(chips - 1, 0, -1):
            row_copy(i, partner(chip, step, chips), to_side).start()

    def near_send(i):
        row_copy(i, chip, 1 - side).start()
        r_ref[i, pl.ds(pl.multiple_of(row * slab, slab), slab), :] = t_ref[i, side, chip]

    def x_send(i):
        row_send(i, 1)
        row_send(i, 0)
        near_send(i)

    tables[0].wait()
    for n in range(pieces):
        load(0, n).wait()
    tables[1].start()
    for s in range(1, stages):
        for n in range(pieces):
            load(s, n).start()
    tables[2].start()
    tables[3].start()
    for small in smalls:
        small.start()
    x_step(0, 0, 1, False)
    pl.semaphore_wait(barrier, rows + cols - 2)
    cross_copy(0).start()

    @pl.when(inner)
    def _():
        cross_copy(1).start()

    @pl.when(jnp.logical_not(inner))
    def _():
        row_send(0, 1)

    near_send(0)
    tables[1].wait()
    x_step(0, 1, chunks, False)
    for j in range(1, chunks):
        x_send(j)
    row_send(0, 0)

    @pl.when(inner)
    def _():
        row_send(0, 1)


    def x_stage(s, carry):
        x_step(s, 0, chunks, True)
        for j in range(chunks):
            x_send(s * chunks + j)
        return carry

    def crosses(step):
        return (partner(col, step, cols) // half) != (col // half)

    def held(step):
        to = partner(col, step, cols)
        late = jnp.logical_and(col * 2 >= cols, jnp.logical_and(to * 2 < cols, to * 4 >= cols))
        return jnp.where(late, HELD, 0)

    def turn(n):
        return jnp.where(jnp.logical_and(early, n < chunks), lax.rem(n + 1, chunks), n)

    def col_send(i):
        for step in range(cols - 1, 0, -1):
            n = i - jnp.where(i < chunks, 0, held(step))
            k = turn(n)
            crossed = jnp.logical_and(jnp.logical_and(k == 0, early), crosses(step))

            due = jnp.logical_and(jnp.logical_or(i < chunks, n >= chunks), n < total)

            @pl.when(jnp.logical_and(due, jnp.logical_not(crossed)))
            def _():
                col_copy(k, step).start()

    def y_modes(ref):
        parts = [ref[pl.ds(g, rows * blocks, stride=SUB), :] for g in range(SUB)]
        high, low = halves(jnp.concatenate(swap_groups(parts), axis=0))
        got = jnp.dot(hy_ref[...], jnp.concatenate([high, high, low], axis=0),
                      preferred_element_type=jnp.float32)
        return got.reshape(cols, share_y, LANES)

    def y_step(i, carry):
        k = turn(i)
        landed(r_ref.at[k, pl.ds(0, (rows - 1) * slab)], recv_row.at[k])
        v_ref[k] = y_modes(r_ref.at[k])
        col_send(i)
        w_ref[k, col] = v_ref[k, col]
        return carry

    def late_send(i, carry):
        col_send(i)
        return carry

    def x_y_stage(s, carry):
        y_step(s - AHEAD, carry)
        return x_stage(s, carry)

    lax.fori_loop(1, AHEAD, x_stage, 0)
    tables[2].wait()
    lax.fori_loop(AHEAD, stages, x_y_stage, 0)
    lax.fori_loop(stages - AHEAD, RELAY, y_step, 0)

    cross_copy(0).wait_recv()
    for step in range(chips - 1, 0, -1):
        relay_copy(partner(chip, step, chips), 0).start()

    @pl.when(inner)
    def _():
        cross_copy(1).wait_recv()
        for step in range(chips - 1, 0, -1):
            relay_copy(partner(chip, step, chips), 1).start()

    @pl.when(jnp.logical_or(side == 1, inner))
    def _():
        relay_copy(chip, 1 - side).start()

    @pl.when(early)
    def _():
        u_ref[pl.ds(pl.multiple_of(row * slab, slab), slab), :] = q_ref[side, chip]

    lax.fori_loop(RELAY, total, y_step, 0)

    lax.fori_loop(total, total + HELD, late_send, 0)

    @pl.when(early)
    def _():
        landed(u_ref.at[pl.ds(0, (rows - 1) * slab)], recv_x.at[0])
        x_ref[...] = y_modes(u_ref)
        base = (col // half) * half
        for step in range(1, half):
            relay_col_copy(base + lax.rem(col - base + step, half)).start()
        w_ref[0, mirror] = x_ref[col]

    tables[3].wait()
    for small in smalls:
        small.wait()
    for n in range(ny // LANES):
        at = slice(n * LANES, (n + 1) * LANES)
        sy_rows[at, :] = jnp.broadcast_to(sy_ref[:, at], (LANES, LANES)).T

    def arrive(f, j):
        for d in range(depths):
            i = (f * depths + d) * chunks + j

            @pl.when(i > 0)
            def _():
                landed(w_ref.at[i, pl.ds(0, cols - 1)], recv_col.at[i])

            def first(near, far, on):
                @pl.when(jnp.logical_and(i == 0, on))
                def _():
                    if near:
                        landed(w_ref.at[i, pl.ds(0, near)], recv_col.at[i])
                    if far:
                        landed(w_ref.at[i, pl.ds(0, far)], recv_x.at[1])

            first(half - 1, half - 1, side == 0)
            odd = 2 * half - 1 - inners
            first(odd, inners - 1, jnp.logical_and(side == 1, inner))
            first(odd, inners, jnp.logical_and(side == 1, jnp.logical_not(inner)))

    def z_step(i, carry):
        f, j = i // chunks, lax.rem(i, chunks)
        arrive(f, j)
        m_ref[i] = modes_of(f, j, chunks, depths, w_ref, hz_ref)
        return carry

    lax.fori_loop(0, (fields - 1) * chunks, z_step, 0)

    def blend_step(x, carry):
        j, k = x // SUB, lax.rem(x, SUB)
        lines_y = sy_rows[pl.ds(pl.multiple_of(col * share_y, share_y), share_y), :]
        lines_y = jnp.concatenate([lines_y] * (nz // LANES), axis=1) + sz_ref[...]
        weight = 1.0 / (1.0 + (sx_ref[row * (chunks * SUB) + x] + lines_y))
        at = pl.ds(pl.multiple_of(k * share_y, share_y), share_y)
        old = [m_ref[f * chunks + j, at, :] for f in range(fields - 1)]
        for f in range(fields):
            gain = (1.0 - weight) * c_ref[f, fields - 1]
            g_ref[f, x] = gain if f < fields - 1 else weight + gain
            mixed = jnp.zeros_like(weight)
            for b in range(fields - 1):
                mixed = mixed + c_ref[f, b] * old[b]
            mixed = (1.0 - weight) * mixed
            o_ref[f, x] = weight * old[f] + mixed if f < fields - 1 else mixed
        return carry

    lax.fori_loop(0, chunks * SUB, blend_step, 0)

    def last_step(j, carry):
        arrive(fields - 1, j)
        last = modes_of(fields - 1, j, chunks, depths, w_ref, hz_ref)
        for k in range(SUB):
            for f in range(fields):
                x = j * SUB + k
                o_ref[f, x] = o_ref[f, x] + g_ref[f, x] * last[k * share_y:(k + 1) * share_y, :]
        return carry

    lax.fori_loop(0, chunks - 1, last_step, 0)
    arrive(fields - 1, chunks - 1)

    landed(t_ref.at[pl.ds(0, total), pl.ds(0, 1)], send_row.at[0])
    landed(t_ref.at[pl.ds(0, total), 1, pl.ds(0, chips - 1)], send_row.at[0])
    landed(v_ref.at[pl.ds(0, total - 1), pl.ds(0, cols - 1)], send_col.at[0])
    cross_copy(0).wait_send()
    landed(q_ref.at[0, pl.ds(0, chips - 1)], send_x.at[1])

    @pl.when(inner)
    def _():
        cross_copy(1).wait_send()
        landed(q_ref.at[1, pl.ds(0, chips - 1)], send_x.at[1])

    @pl.when(jnp.logical_or(side == 1, inner))
    def _():
        landed(q_ref.at[0, 0], send_x.at[1])

    @pl.when(jnp.logical_not(early))
    def _():
        landed(v_ref.at[0, pl.ds(0, cols - 1)], send_col.at[0])

    if half > 1:
        @pl.when(early)
        def _():
            landed(v_ref.at[0, pl.ds(0, half - 1)], send_col.at[0])
            landed(x_ref.at[pl.ds(0, half - 1)], send_x.at[2])


def finish(depths, o_ref, g_ref, w_ref, hz_ref, out_hbm, e_ref, sem):
    fields, share_x, share_y, nz = o_ref.shape
    ready = share_x - SUB
    early = [pltpu.make_async_copy(o_ref.at[f, pl.ds(0, ready)], out_hbm.at[f, pl.ds(0, ready)], sem.at[f])
             for f in range(fields)]
    for copy in early:
        copy.start()
    last = modes_of(fields - 1, share_x // SUB - 1, share_x // SUB, depths, w_ref, hz_ref)
    late = []
    for f in range(fields):
        for k in range(SUB):
            x = ready + k
            e_ref[f, k] = o_ref[f, x] + g_ref[f, x] * last[k * share_y:(k + 1) * share_y, :]
        late.append(pltpu.make_async_copy(e_ref.at[f], out_hbm.at[f, pl.ds(ready, SUB)], sem.at[fields + f]))
        late[-1].start()
    for copy in early + late:
        copy.wait()


def local(rows, cols, species, coupling, symbol_x, symbol_y, symbol_z):
    fields, nx, near_y, near_z = species.shape
    ny, nz = near_y * rows, near_z * cols
    share_x, share_y = nx // rows, ny // cols
    depths, blocks, chunks = near_z // DEPTH, near_y // SUB, share_x // SUB
    stages = fields * depths
    total = stages * chunks

    order = np.arange(nx).reshape(rows // 2, 2, chunks, SUB).transpose(2, 1, 0, 3).reshape(-1)
    high, low = halves_of(mode_table(nx)[order])
    hx = np.concatenate([high, low, high], axis=1)
    order = np.arange(ny).reshape(rows, blocks, SUB).transpose(2, 0, 1).reshape(-1)
    high, low = halves_of(mode_table(ny)[:, order])
    hy = np.concatenate([high, low, high], axis=1)
    high, low = halves_of(mode_table(nz))
    hz = np.concatenate([np.concatenate([high, low], axis=1),
                         np.concatenate([high, np.zeros_like(low)], axis=1)], axis=0)

    lines = jnp.transpose(species, (0, 2, 3, 1))
    vmem = pl.BlockSpec(memory_space=pltpu.VMEM)
    hbm = pl.BlockSpec(memory_space=pltpu.HBM)
    dma = pltpu.SemaphoreType.DMA
    f32 = jnp.float32
    out = (fields, share_x, share_y, nz)
    kept = 4 * (2 * fields * share_x * share_y * nz + total * cols * share_y * LANES) + 2 * hz.size
    held = pl.pallas_call(
        functools.partial(kernel, (rows, cols, fields, nx, ny, nz)),
        out_shape=[
            pltpu.VMEM(out, f32),
            pltpu.VMEM(out, f32),
            pltpu.VMEM((total, cols, share_y, LANES), f32),
            pltpu.VMEM(hz.shape, hz.dtype),
        ],
        in_specs=[hbm] * 8,
        out_specs=[vmem] * 4,
        scratch_shapes=[
            pltpu.SMEM(coupling.shape, f32),
            pltpu.SMEM(symbol_x.shape, f32),
            pltpu.VMEM((1, ny), f32),
            pltpu.VMEM((1, nz), f32),
            pltpu.VMEM((stages, near_y, DEPTH, nx), f32),
            pltpu.VMEM(hx.shape, hx.dtype),
            pltpu.VMEM(hy.shape, hy.dtype),
            pltpu.VMEM((ny, LANES), f32),
            pltpu.VMEM((max((fields - 1) * chunks, 1), SUB * share_y, nz), f32),
            pltpu.VMEM((total, 2, rows // 2, blocks * SUB, LANES), f32),
            pltpu.VMEM((total, rows * blocks * SUB, LANES), f32),
            pltpu.VMEM((total, cols, share_y, LANES), f32),
            pltpu.VMEM((2, rows // 2, blocks * SUB, LANES), f32),
            pltpu.VMEM((rows * blocks * SUB, LANES), f32),
            pltpu.VMEM((cols, share_y, LANES), f32),
            dma((stages, blocks // 2)), dma((4,)), dma((4,)),
            dma((1,)), dma((total,)), dma((1,)), dma((total,)), dma((3,)), dma((4,)),
        ],
        compiler_params=pltpu.CompilerParams(
            collective_id=0, has_side_effects=True, vmem_limit_bytes=60 * 2**20 - kept),
    )(coupling, symbol_x, lines, jnp.asarray(hx), jnp.asarray(hy), jnp.asarray(hz),
      symbol_y[None, :], symbol_z[None, :])
    return pl.pallas_call(
        functools.partial(finish, depths),
        out_shape=jax.ShapeDtypeStruct(out, f32),
        in_specs=[vmem] * 4,
        out_specs=hbm,
        scratch_shapes=[pltpu.VMEM((fields, SUB, share_y, nz), f32), dma((2 * fields,))],
        compiler_params=pltpu.CompilerParams(vmem_limit_bytes=16 * 2**20),
    )(*held)


def solution(mesh):
    return jax.shard_map(
        functools.partial(local, mesh.shape["row"], mesh.shape["col"]),
        mesh=mesh,
        in_specs=(P(None, None, "row", "col"), P(), P(), P(), P()),
        out_specs=P(None, "row", "col", None),
        check_vma=False,
    )
```

```python
import functools

import jax
import jax.numpy as jnp
import numpy as np
from jax import lax
from jax.experimental import pallas as pl
from jax.experimental.pallas import tpu as pltpu
from jax.sharding import PartitionSpec as P

MESH = pl.DeviceIdType.MESH
LANES = 128
SUB = 8
DEPTH = LANES // SUB
HELD = 6
RELAY = 4
AHEAD = 2


def mode_table(count):
    rank = np.arange(1, count + 1)
    angle = np.pi / (count + 1) * ((rank[:, None] * rank[None, :]) % (2 * count + 2))
    return (np.sin(angle) * np.sqrt(2.0 / (count + 1))).astype(np.float32)


def halves_of(table):
    high = table.astype(jnp.bfloat16)
    low = (table - high.astype(np.float32)).astype(jnp.bfloat16)
    return high, low


def halves(values):
    high = values.astype(jnp.bfloat16)
    low = (values - high.astype(jnp.float32)).astype(jnp.bfloat16)
    return high, low


def partner(me, step, count):
    if count & (count - 1):
        return lax.rem(me + step, count)
    other, bit = me, 1
    while bit < count:
        if step & bit:
            other = other + bit * (1 - 2 * lax.rem(me // bit, 2))
        bit *= 2
    return other


def swap_groups(parts):
    parts = list(parts)
    count = len(parts)
    width = LANES // count
    lane = lax.broadcasted_iota(jnp.int32, parts[0].shape, 1)
    step = count // 2
    while step:
        keep = lax.rem(lane // (width * step), 2) == 0
        for first in range(count):
            if first & step:
                continue
            a, b = parts[first], parts[first + step]
            parts[first] = jnp.where(keep, a, pltpu.roll(b, width * step, 1))
            parts[first + step] = jnp.where(keep, pltpu.roll(a, LANES - width * step, 1), b)
        step //= 2
    return parts


def modes_of(f, j, chunks, depths, w_ref, hz_ref):
    cols, nz = w_ref.shape[1], hz_ref.shape[1] // 2
    parts = [w_ref[(f * depths + p % depths) * chunks + j, p // depths] for p in range(cols * depths)]
    tiles = [swap_groups(parts[p:p + SUB]) for p in range(0, cols * depths, SUB)]
    lines = [jnp.concatenate([tile[k] for tile in tiles], axis=1) for k in range(SUB)]
    high, low = halves(jnp.concatenate(lines, axis=0))
    got = jnp.dot(jnp.concatenate([high, low], axis=1), hz_ref[...],
                  preferred_element_type=jnp.float32)
    return got[:, :nz] + got[:, nz:]


def kernel(sizes, c_hbm, sx_hbm, a_hbm, hx_hbm, hy_hbm, hz_hbm, sy_hbm, sz_hbm,
           o_ref, g_ref, w_ref, hz_ref,
           c_ref, sx_ref, sy_ref, sz_ref, a_ref, hx_ref, hy_ref, sy_rows, m_ref,
           t_ref, r_ref, v_ref, q_ref, u_ref, x_ref,
           load_a, load_h, load_s, send_row, recv_row, send_col, recv_col, send_x, recv_x):
    rows, cols, fields, nx, ny, nz = sizes
    share_y = ny // cols
    near_y = ny // rows
    depths = nz // cols // DEPTH
    blocks = near_y // SUB
    chunks = nx // rows // SUB
    stages = fields * depths
    total = stages * chunks
    slab = blocks * SUB
    span = rows * SUB
    row, col = lax.axis_index("row"), lax.axis_index("col")
    chips, half = rows // 2, cols // 2
    chip, side = row // 2, lax.rem(row, 2)
    mirror = cols - 1 - col
    inner = jnp.logical_and(col * 4 >= cols, col * 4 < 3 * cols)
    early = jnp.logical_or(side == 0, inner)
    inners = half // 2
    per_dot = 2
    width = per_dot * LANES
    pieces = blocks // per_dot

    def load(s, n):
        f, d = s // depths, s % depths
        lines = width // DEPTH
        return pltpu.make_async_copy(
            a_hbm.at[f, pl.ds(n * lines, lines), pl.ds(d * DEPTH, DEPTH)],
            a_ref.at[s, pl.ds(n * lines, lines)], load_a.at[s, n])

    tables = [pltpu.make_async_copy(src, dst, load_h.at[n]) for n, (src, dst) in enumerate(
        ((hx_hbm.at[pl.ds(0, span)], hx_ref.at[pl.ds(0, span)]),
         (hx_hbm.at[pl.ds(span, nx - span)], hx_ref.at[pl.ds(span, nx - span)]),
         (hy_hbm, hy_ref), (hz_hbm, hz_ref)))]
    smalls = [pltpu.make_async_copy(src, dst, load_s.at[n]) for n, (src, dst) in enumerate(
        ((c_hbm, c_ref), (sx_hbm, sx_ref), (sy_hbm, sy_ref), (sz_hbm, sz_ref)))]
    barrier = pltpu.get_barrier_semaphore()
    tables[0].start()
    for n in range(pieces):
        load(0, n).start()
    for step in range(1, rows):
        pl.semaphore_signal(barrier, inc=1, device_id={"row": partner(row, step, rows)}, device_id_type=MESH)
    for step in range(1, cols):
        pl.semaphore_signal(barrier, inc=1, device_id={"col": partner(col, step, cols)}, device_id_type=MESH)

    def row_copy(i, to_chip, to_side):
        return pltpu.make_async_remote_copy(
            src_ref=t_ref.at[i, to_side, to_chip], dst_ref=r_ref.at[i, pl.ds(row * slab, slab)],
            send_sem=send_row.at[0], recv_sem=recv_row.at[i],
            device_id={"row": 2 * to_chip + to_side}, device_id_type=MESH)

    def cross_copy(to_side):
        return pltpu.make_async_remote_copy(
            src_ref=t_ref.at[0, to_side], dst_ref=q_ref.at[to_side],
            send_sem=send_x.at[0], recv_sem=recv_x.at[2 + to_side],
            device_id={"col": mirror}, device_id_type=MESH)

    def relay_copy(to_chip, to_side):
        return pltpu.make_async_remote_copy(
            src_ref=q_ref.at[to_side, to_chip], dst_ref=u_ref.at[pl.ds(row * slab, slab)],
            send_sem=send_x.at[1], recv_sem=recv_x.at[0],
            device_id={"row": 2 * to_chip + to_side}, device_id_type=MESH)

    def relay_col_copy(to):
        return pltpu.make_async_remote_copy(
            src_ref=x_ref.at[to], dst_ref=w_ref.at[0, mirror],
            send_sem=send_x.at[2], recv_sem=recv_x.at[1],
            device_id={"col": to}, device_id_type=MESH)

    def col_copy(i, step):
        to = partner(col, step, cols)
        return pltpu.make_async_remote_copy(
            src_ref=v_ref.at[i, to], dst_ref=w_ref.at[i, col],
            send_sem=send_col.at[0], recv_sem=recv_col.at[i],
            device_id={"col": to}, device_id_type=MESH)

    def landed(ref, sem):
        pltpu.make_async_copy(ref, ref, sem).wait()

    def x_step(s, low_j, top_j, waits):
        for n in range(pieces):
            if waits:
                load(s, n).wait()
            lines = width // DEPTH
            high, low = halves(a_ref[s, n * lines:(n + 1) * lines].reshape(width, nx))
            part = lax.dot_general(
                hx_ref[low_j * span:top_j * span, :], jnp.concatenate([high, high, low], axis=1),
                (((1,), (1,)), ((), ())), preferred_element_type=jnp.float32)
            part = part.reshape(top_j - low_j, 2, chips, SUB, width)
            for j in range(low_j, top_j):
                for b in range(per_dot):
                    at = (n * per_dot + b) * SUB
                    t_ref[s * chunks + j, :, :, at:at + SUB, :] = part[
                        j - low_j, :, :, :, b * LANES:(b + 1) * LANES]

    def row_send(i, to_side):
        for step in range(chips - 1, 0, -1):
            row_copy(i, partner(chip, step, chips), to_side).start()

    def near_send(i):
        row_copy(i, chip, 1 - side).start()
        r_ref[i, pl.ds(pl.multiple_of(row * slab, slab), slab), :] = t_ref[i, side, chip]

    def x_send(i, j):
        row_send(i, j % 2)
        row_send(i, 1 - j % 2)
        near_send(i)

    tables[0].wait()
    for n in range(pieces):
        load(0, n).wait()
    tables[1].start()
    for s in range(1, stages):
        for n in range(pieces):
            load(s, n).start()
    tables[2].start()
    tables[3].start()
    for small in smalls:
        small.start()
    x_step(0, 0, 1, False)
    pl.semaphore_wait(barrier, rows + cols - 2)
    cross_copy(0).start()

    @pl.when(inner)
    def _():
        cross_copy(1).start()

    @pl.when(jnp.logical_not(inner))
    def _():
        row_send(0, 1)

    near_send(0)
    tables[1].wait()
    x_step(0, 1, chunks, False)
    for j in range(1, chunks):
        x_send(j, j)
    row_send(0, 0)

    @pl.when(inner)
    def _():
        row_send(0, 1)


    def x_stage(s, carry):
        x_step(s, 0, chunks, True)
        for j in range(chunks):
            x_send(s * chunks + j, j)
        return carry

    def crosses(step):
        return (partner(col, step, cols) // half) != (col // half)

    def held(step):
        to = partner(col, step, cols)
        late = jnp.logical_and(col * 2 >= cols, jnp.logical_and(to * 2 < cols, to * 4 >= cols))
        return jnp.where(late, HELD, 0)

    def turn(n):
        return jnp.where(jnp.logical_and(early, n < chunks), lax.rem(n + 1, chunks), n)

    def col_send(i):
        for step in range(cols - 1, 0, -1):
            n = i - jnp.where(i < chunks, 0, held(step))
            k = turn(n)
            crossed = jnp.logical_and(jnp.logical_and(k == 0, early), crosses(step))

            due = jnp.logical_and(jnp.logical_or(i < chunks, n >= chunks), n < total)

            @pl.when(jnp.logical_and(due, jnp.logical_not(crossed)))
            def _():
                col_copy(k, step).start()

    def y_modes(ref):
        parts = [ref[pl.ds(g, rows * blocks, stride=SUB), :] for g in range(SUB)]
        high, low = halves(jnp.concatenate(swap_groups(parts), axis=0))
        got = jnp.dot(hy_ref[...], jnp.concatenate([high, high, low], axis=0),
                      preferred_element_type=jnp.float32)
        return got.reshape(cols, share_y, LANES)

    def y_step(i, carry):
        k = turn(i)
        landed(r_ref.at[k, pl.ds(0, (rows - 1) * slab)], recv_row.at[k])
        v_ref[k] = y_modes(r_ref.at[k])
        col_send(i)
        w_ref[k, col] = v_ref[k, col]
        return carry

    def late_send(i, carry):
        col_send(i)
        return carry

    def x_y_stage(s, carry):
        y_step(s - AHEAD, carry)
        return x_stage(s, carry)

    lax.fori_loop(1, AHEAD, x_stage, 0)
    tables[2].wait()
    lax.fori_loop(AHEAD, stages, x_y_stage, 0)
    lax.fori_loop(stages - AHEAD, RELAY, y_step, 0)

    cross_copy(0).wait_recv()
    for step in range(chips - 1, 0, -1):
        relay_copy(partner(chip, step, chips), 0).start()

    @pl.when(inner)
    def _():
        cross_copy(1).wait_recv()
        for step in range(chips - 1, 0, -1):
            relay_copy(partner(chip, step, chips), 1).start()

    @pl.when(jnp.logical_or(side == 1, inner))
    def _():
        relay_copy(chip, 1 - side).start()

    @pl.when(early)
    def _():
        u_ref[pl.ds(pl.multiple_of(row * slab, slab), slab), :] = q_ref[side, chip]

    lax.fori_loop(RELAY, total, y_step, 0)

    lax.fori_loop(total, total + HELD, late_send, 0)

    @pl.when(early)
    def _():
        landed(u_ref.at[pl.ds(0, (rows - 1) * slab)], recv_x.at[0])
        x_ref[...] = y_modes(u_ref)
        base = (col // half) * half
        for step in range(1, half):
            relay_col_copy(base + lax.rem(col - base + step, half)).start()
        w_ref[0, mirror] = x_ref[col]

    tables[3].wait()
    for small in smalls:
        small.wait()
    for n in range(ny // LANES):
        at = slice(n * LANES, (n + 1) * LANES)
        sy_rows[at, :] = jnp.broadcast_to(sy_ref[:, at], (LANES, LANES)).T

    def arrive(f, j):
        for d in range(depths):
            i = (f * depths + d) * chunks + j

            @pl.when(i > 0)
            def _():
                landed(w_ref.at[i, pl.ds(0, cols - 1)], recv_col.at[i])

            def first(near, far, on):
                @pl.when(jnp.logical_and(i == 0, on))
                def _():
                    if near:
                        landed(w_ref.at[i, pl.ds(0, near)], recv_col.at[i])
                    if far:
                        landed(w_ref.at[i, pl.ds(0, far)], recv_x.at[1])

            first(half - 1, half - 1, side == 0)
            odd = 2 * half - 1 - inners
            first(odd, inners - 1, jnp.logical_and(side == 1, inner))
            first(odd, inners, jnp.logical_and(side == 1, jnp.logical_not(inner)))

    def z_step(i, carry):
        f, j = i // chunks, lax.rem(i, chunks)
        arrive(f, j)
        m_ref[i] = modes_of(f, j, chunks, depths, w_ref, hz_ref)
        return carry

    lax.fori_loop(0, (fields - 1) * chunks, z_step, 0)

    def blend_step(x, carry):
        j, k = x // SUB, lax.rem(x, SUB)
        lines_y = sy_rows[pl.ds(pl.multiple_of(col * share_y, share_y), share_y), :]
        lines_y = jnp.concatenate([lines_y] * (nz // LANES), axis=1) + sz_ref[...]
        weight = 1.0 / (1.0 + (sx_ref[row * (chunks * SUB) + x] + lines_y))
        at = pl.ds(pl.multiple_of(k * share_y, share_y), share_y)
        old = [m_ref[f * chunks + j, at, :] for f in range(fields - 1)]
        for f in range(fields):
            gain = (1.0 - weight) * c_ref[f, fields - 1]
            g_ref[f, x] = gain if f < fields - 1 else weight + gain
            mixed = jnp.zeros_like(weight)
            for b in range(fields - 1):
                mixed = mixed + c_ref[f, b] * old[b]
            mixed = (1.0 - weight) * mixed
            o_ref[f, x] = weight * old[f] + mixed if f < fields - 1 else mixed
        return carry

    lax.fori_loop(0, chunks * SUB, blend_step, 0)

    def last_step(j, carry):
        arrive(fields - 1, j)
        last = modes_of(fields - 1, j, chunks, depths, w_ref, hz_ref)
        for k in range(SUB):
            for f in range(fields):
                x = j * SUB + k
                o_ref[f, x] = o_ref[f, x] + g_ref[f, x] * last[k * share_y:(k + 1) * share_y, :]
        return carry

    lax.fori_loop(0, chunks - 1, last_step, 0)
    arrive(fields - 1, chunks - 1)

    landed(t_ref.at[pl.ds(0, total), pl.ds(0, 1)], send_row.at[0])
    landed(t_ref.at[pl.ds(0, total), 1, pl.ds(0, chips - 1)], send_row.at[0])
    landed(v_ref.at[pl.ds(0, total - 1), pl.ds(0, cols - 1)], send_col.at[0])
    cross_copy(0).wait_send()
    landed(q_ref.at[0, pl.ds(0, chips - 1)], send_x.at[1])

    @pl.when(inner)
    def _():
        cross_copy(1).wait_send()
        landed(q_ref.at[1, pl.ds(0, chips - 1)], send_x.at[1])

    @pl.when(jnp.logical_or(side == 1, inner))
    def _():
        landed(q_ref.at[0, 0], send_x.at[1])

    @pl.when(jnp.logical_not(early))
    def _():
        landed(v_ref.at[0, pl.ds(0, cols - 1)], send_col.at[0])

    if half > 1:
        @pl.when(early)
        def _():
            landed(v_ref.at[0, pl.ds(0, half - 1)], send_col.at[0])
            landed(x_ref.at[pl.ds(0, half - 1)], send_x.at[2])


def finish(depths, o_ref, g_ref, w_ref, hz_ref, out_hbm, e_ref, sem):
    fields, share_x, share_y, nz = o_ref.shape
    ready = share_x - SUB
    early = [pltpu.make_async_copy(o_ref.at[f, pl.ds(0, ready)], out_hbm.at[f, pl.ds(0, ready)], sem.at[f])
             for f in range(fields)]
    for copy in early:
        copy.start()
    last = modes_of(fields - 1, share_x // SUB - 1, share_x // SUB, depths, w_ref, hz_ref)
    late = []
    for f in range(fields):
        for k in range(SUB):
            x = ready + k
            e_ref[f, k] = o_ref[f, x] + g_ref[f, x] * last[k * share_y:(k + 1) * share_y, :]
        late.append(pltpu.make_async_copy(e_ref.at[f], out_hbm.at[f, pl.ds(ready, SUB)], sem.at[fields + f]))
        late[-1].start()
    for copy in early + late:
        copy.wait()


def local(rows, cols, species, coupling, symbol_x, symbol_y, symbol_z):
    fields, nx, near_y, near_z = species.shape
    ny, nz = near_y * rows, near_z * cols
    share_x, share_y = nx // rows, ny // cols
    depths, blocks, chunks = near_z // DEPTH, near_y // SUB, share_x // SUB
    stages = fields * depths
    total = stages * chunks

    order = np.arange(nx).reshape(rows // 2, 2, chunks, SUB).transpose(2, 1, 0, 3).reshape(-1)
    high, low = halves_of(mode_table(nx)[order])
    hx = np.concatenate([high, low, high], axis=1)
    order = np.arange(ny).reshape(rows, blocks, SUB).transpose(2, 0, 1).reshape(-1)
    high, low = halves_of(mode_table(ny)[:, order])
    hy = np.concatenate([high, low, high], axis=1)
    high, low = halves_of(mode_table(nz))
    hz = np.concatenate([np.concatenate([high, low], axis=1),
                         np.concatenate([high, np.zeros_like(low)], axis=1)], axis=0)

    lines = jnp.transpose(species, (0, 2, 3, 1))
    vmem = pl.BlockSpec(memory_space=pltpu.VMEM)
    hbm = pl.BlockSpec(memory_space=pltpu.HBM)
    dma = pltpu.SemaphoreType.DMA
    f32 = jnp.float32
    out = (fields, share_x, share_y, nz)
    kept = 4 * (2 * fields * share_x * share_y * nz + total * cols * share_y * LANES) + 2 * hz.size
    held = pl.pallas_call(
        functools.partial(kernel, (rows, cols, fields, nx, ny, nz)),
        out_shape=[
            pltpu.VMEM(out, f32),
            pltpu.VMEM(out, f32),
            pltpu.VMEM((total, cols, share_y, LANES), f32),
            pltpu.VMEM(hz.shape, hz.dtype),
        ],
        in_specs=[hbm] * 8,
        out_specs=[vmem] * 4,
        scratch_shapes=[
            pltpu.SMEM(coupling.shape, f32),
            pltpu.SMEM(symbol_x.shape, f32),
            pltpu.VMEM((1, ny), f32),
            pltpu.VMEM((1, nz), f32),
            pltpu.VMEM((stages, near_y, DEPTH, nx), f32),
            pltpu.VMEM(hx.shape, hx.dtype),
            pltpu.VMEM(hy.shape, hy.dtype),
            pltpu.VMEM((ny, LANES), f32),
            pltpu.VMEM((max((fields - 1) * chunks, 1), SUB * share_y, nz), f32),
            pltpu.VMEM((total, 2, rows // 2, blocks * SUB, LANES), f32),
            pltpu.VMEM((total, rows * blocks * SUB, LANES), f32),
            pltpu.VMEM((total, cols, share_y, LANES), f32),
            pltpu.VMEM((2, rows // 2, blocks * SUB, LANES), f32),
            pltpu.VMEM((rows * blocks * SUB, LANES), f32),
            pltpu.VMEM((cols, share_y, LANES), f32),
            dma((stages, blocks // 2)), dma((4,)), dma((4,)),
            dma((1,)), dma((total,)), dma((1,)), dma((total,)), dma((3,)), dma((4,)),
        ],
        compiler_params=pltpu.CompilerParams(
            collective_id=0, has_side_effects=True, vmem_limit_bytes=60 * 2**20 - kept),
    )(coupling, symbol_x, lines, jnp.asarray(hx), jnp.asarray(hy), jnp.asarray(hz),
      symbol_y[None, :], symbol_z[None, :])
    return pl.pallas_call(
        functools.partial(finish, depths),
        out_shape=jax.ShapeDtypeStruct(out, f32),
        in_specs=[vmem] * 4,
        out_specs=hbm,
        scratch_shapes=[pltpu.VMEM((fields, SUB, share_y, nz), f32), dma((2 * fields,))],
        compiler_params=pltpu.CompilerParams(vmem_limit_bytes=16 * 2**20),
    )(*held)


def solution(mesh):
    return jax.shard_map(
        functools.partial(local, mesh.shape["row"], mesh.shape["col"]),
        mesh=mesh,
        in_specs=(P(None, None, "row", "col"), P(), P(), P(), P()),
        out_specs=P(None, "row", "col", None),
        check_vma=False,
    )
```
